32 devices in a mesh: dp: 8 (over y, x, core), mp: 4 (over z).
Axes of the slice: x: 2, y: 2, z: 4, core: 2. Of those that a mesh axis runs over, the one named last changes fastest.
Arguments:
- patches: bfloat16 [24576, 3072], P(('dp', 'mp')), may hold values from -6 to 6
- wavelengths: int32 [12], replicated, may hold values from 400 to 2499
- counts: int32 [384], P('dp'), may hold values from 1 to 64, 18432 in all
- positions: int32 [384, 64], P(('dp', 'mp')), may hold values from 0 to 195, as said below
- relation: bfloat16 [128, 384], replicated, may hold values from -1 to 1
- blending: bfloat16 [128, 128], replicated, may hold values from -0.5 to 0.5
- widening: bfloat16 [128, 2048], replicated, may hold values from -0.5 to 0.5
- narrowing: bfloat16 [2048, 128], replicated, may hold values from -0.125 to 0.125
- generator: bfloat16 [256, 128, 768], P(('dp', 'mp')), may hold values from -0.009765625 to 0.009765625
- shifting: bfloat16 [128, 768], replicated, may hold values from -0.5 to 0.5
- scaling: bfloat16 [768], replicated, may hold values from 0.25 to 1.75
- centring: bfloat16 [768], replicated, may hold values from -1.5 to 1.5
- attending: bfloat16 [768, 3, 768], P(None, None, 'mp'), may hold values from -0.21875 to 0.21875
- offsets: bfloat16 [2, 768], P(None, 'mp'), may hold values from -1.5 to 1.5
- merging: bfloat16 [768, 768], P('mp'), may hold values from -0.875 to 0.875
- lifting: bfloat16 [768], replicated, may hold values from -1.5 to 1.5
- rescaling: bfloat16 [768], replicated, may hold values from 0.25 to 1.75
- recentring: bfloat16 [768], replicated, may hold values from -1.5 to 1.5
- expanding: bfloat16 [768, 3072], P(None, 'mp'), may hold values from -0.21875 to 0.21875
- priming: bfloat16 [3072], P('mp'), may hold values from -1.5 to 1.5
- shrinking: bfloat16 [3072, 768], P('mp'), may hold values from -0.109375 to 0.109375
- settling: bfloat16 [768], replicated, may hold values from -1.5 to 1.5
- cotangent: bfloat16 [24576, 768], P(('dp', 'mp')), may hold values from -6 to 6
Outputs:
- layer_out: bfloat16 [24576, 768], P(('dp', 'mp'))
- patches_grad: float32 [24576, 3072], P(('dp', 'mp'))
- relation_grad: float32 [128, 384], replicated
- blending_grad: float32 [128, 128], replicated
- widening_grad: float32 [128, 2048], replicated
- narrowing_grad: float32 [2048, 128], replicated
- generator_grad: float32 [256, 128, 768], P(('dp', 'mp'))
- shifting_grad: float32 [128, 768], replicated
- scaling_grad: float32 [768], replicated
- centring_grad: float32 [768], replicated
- attending_grad: float32 [768, 3, 768], P(None, None, 'mp')
- offsets_grad: float32 [2, 768], P(None, 'mp')
- merging_grad: float32 [768, 768], P('mp')
- lifting_grad: float32 [768], replicated
- rescaling_grad: float32 [768], replicated
- recentring_grad: float32 [768], replicated
- expanding_grad: float32 [768, 3072], P(None, 'mp')
- priming_grad: float32 [3072], P('mp')
- shrinking_grad: float32 [3072, 768], P('mp')
- settling_grad: float32 [768], replicated
The draws below stay inside these ranges and needn't reach their ends.
Inputs may be any that keep to these rules, and one draw needn't show every extreme that they name: Image i keeps its first counts[i] slots; the counts of all images sum to 18432, and some image keeps all 64. The 64 positions of an image are distinct cells of its 14 x 14 grid of patches.
All inputs are finite; a program needn't handle non-finite values. No bound on the sum of `counts` on one device may be relied on, other than what follows from the above.
Results may differ from the reference program's by a relative error of at most 0.025.
Values may be sent and summed in bfloat16 or wider, within the bound.
A program may use at most 192 MiB of HBM per device.

```python
import math
import jax
import jax.numpy as jnp
import numpy as np
from jax import lax

D = 768
HEADS = 12
FF = 3072
HYP = 128
HYP_HEADS = 4
HYP_FF = 2048
PIX = 256
BANDS = 12
SLOTS = 64
GRID_SIDE = 14
IMG_DEV = 48
IMAGES = 384
TOKENS = 24576
N_DP = 8


def draw_positions(key, part):
    image_keys = jax.random.split(jax.random.fold_in(key, 17), IMAGES)

    def one_image(image_key):
        return jax.random.permutation(image_key, GRID_SIDE * GRID_SIDE)[:SLOTS]
    return jax.vmap(one_image)(image_keys).astype(jnp.int32)


def place_ends(values, key, low, high):
    index_at = [jax.random.randint(jax.random.fold_in(key, axis), (), 0, length) for axis, length in enumerate(values.shape)]
    longest = values.shape.index(max(values.shape))
    next_to = index_at[:longest] + [(index_at[longest] + 1) % values.shape[longest]] + index_at[longest + 1:]
    return values.at[tuple(index_at)].set(low).at[tuple(next_to)].set(high)


def steps_of(stream_key, dims, shards, low, top_value):
    def one(axis_at, blocks):
        steps = jax.random.uniform(jax.random.fold_in(jax.random.fold_in(stream_key, 6), axis_at), (blocks,), jnp.float32, low / len(shards), top_value / len(shards))
        return jnp.repeat(jnp.exp(steps), dims[axis_at] // blocks).reshape((-1,) + (1,) * (len(dims) - axis_at - 1))

    factor_of = one(*shards[0])
    for cut in shards[1:]:
        factor_of = factor_of * one(*cut)
    return factor_of


def profile(count, total, bound, lean):
    portions = [(1 << 20) // math.isqrt(standing ** lean) + 1 for standing in range(2, count + 1)]
    rest, given = total - bound - (count - 1), [1] * (count - 1)
    while rest > 0:
        free = [i for i in range(count - 1) if given[i] < bound]
        whole, remaining = sum([portions[i] for i in free]), rest
        for i in free:
            extra = min(bound - given[i], max(1, remaining * portions[i] // whole), rest)
            given[i] = given[i] + extra
            rest = rest - extra
    return np.array([bound] + given)


def ragged_sizes(rng, amount, total, reach, slope):
    if amount == 2:
        one = jax.random.randint(rng, (), max(1, total - reach), min(reach, total - 1) + 1)
        return jnp.stack([one, total - one])
    lengths = jnp.asarray(profile(amount, total, reach, slope), jnp.int32)
    pairs = (amount - 1) // 2
    donor, taker = lengths[1:1 + 2 * pairs:2], lengths[2:2 + 2 * pairs:2]
    room = jnp.minimum(donor - 1, reach - taker)
    moved = jax.random.randint(jax.random.fold_in(rng, 1), (pairs,), 0, 1 << 20) % (room + 1)
    lengths = lengths.at[1:1 + 2 * pairs:2].set(donor - moved).at[2:2 + 2 * pairs:2].set(taker + moved)
    return lengths[jax.random.permutation(jax.random.fold_in(rng, 2), amount)]


def noise(rng, dims, scale, most, cuts=(), kind=jnp.bfloat16):
    values = scale * jax.random.normal(rng, dims, jnp.float32)
    if cuts:
        values = values * steps_of(rng, dims, cuts, -0.22, 0.18)
    return jnp.clip(values, -most, most).astype(kind)


def setup_inputs(seed: int = 0) -> dict:
    key_list = jax.random.split(jax.random.key(seed), 24)
    return {
        "patches": noise(key_list[0], (TOKENS, PIX * BANDS), 1.0, 6.0, ((0, 32),)),
        "wavelengths": place_ends(jax.random.randint(key_list[1], (BANDS,), 400, 2500), jax.random.fold_in(key_list[1], 1), 400, 2499).astype(jnp.int32),
        "counts": ragged_sizes(key_list[2], IMAGES, IMAGES * SLOTS * 3 // 4, SLOTS, 2).astype(jnp.int32),
        "positions": draw_positions(jax.random.fold_in(key_list[23], 71), 0),
        "relation": noise(key_list[4], (HYP, 3 * HYP), (HYP // 4) ** -0.5, 1.0),
        "blending": noise(key_list[5], (HYP, HYP), HYP ** -0.5, 0.5),
        "widening": noise(key_list[6], (HYP, HYP_FF), HYP ** -0.5, 0.5),
        "narrowing": noise(key_list[7], (HYP_FF, HYP), HYP_FF ** -0.5, 0.125),
        "generator": noise(key_list[8], (PIX, HYP, D), (HYP * PIX * BANDS) ** -0.5, 0.009765625, ((0, 32),)),
        "shifting": noise(key_list[9], (HYP, D), HYP ** -0.5, 0.5),
        "scaling": jnp.clip(1.0 + 0.15 * jax.random.normal(key_list[10], (D,), jnp.float32), 0.25, 1.75).astype(jnp.bfloat16),
        "centring": noise(key_list[11], (D,), 0.3, 1.5),
        "attending": noise(key_list[12], (D, 3, D), D ** -0.5, 0.21875, ((2, 4),)),
        "offsets": noise(key_list[13], (2, D), 0.3, 1.5, ((1, 4),)),
        "merging": noise(key_list[14], (D, D), (D // 16) ** -0.5, 0.875, ((0, 4),)),
        "lifting": noise(key_list[15], (D,), 0.3, 1.5),
        "rescaling": jnp.clip(1.0 + 0.15 * jax.random.normal(key_list[16], (D,), jnp.float32), 0.25, 1.75).astype(jnp.bfloat16),
        "recentring": noise(key_list[17], (D,), 0.3, 1.5),
        "expanding": noise(key_list[18], (D, FF), D ** -0.5, 0.21875, ((1, 4),)),
        "priming": noise(key_list[19], (FF,), 0.3, 1.5, ((0, 4),)),
        "shrinking": noise(key_list[20], (FF, D), FF ** -0.5, 0.109375, ((0, 4),)),
        "settling": noise(key_list[21], (D,), 0.3, 1.5),
        "cotangent": noise(key_list[22], (TOKENS, D), 1.0, 6.0, ((0, 32),)),
    }


@jax.custom_vjp
def low(v):
    return lax.optimization_barrier(v.astype(jnp.bfloat16)).astype(jnp.float32)

@jax.custom_vjp
def low_back(v):
    return v

def low_keep(v):
    return (low(v), None)

def low_pass(kept, grad):
    return (grad,)

def back_keep(v):
    return (v, None)

def back_low(kept, grad):
    return (low(grad),)
low.defvjp(low_keep, low_pass)
low_back.defvjp(back_keep, back_low)

def both_round(values):
    return low_back(low(values))

def normalize(values, epsilon):
    center = values - lax.optimization_barrier(jnp.mean(values, axis=-1, keepdims=True))
    return center * lax.rsqrt(lax.optimization_barrier(jnp.mean(center * center, axis=-1, keepdims=True)) + epsilon)

def wave_embed(wavelengths, columns):
    halfway = columns // 2
    omegas = 10000.0 ** (-jnp.arange(halfway, dtype=jnp.float32) / halfway)
    angles = wavelengths.astype(jnp.float32)[:, None] * 0.01 * omegas[None, :]
    return jnp.concatenate([jnp.sin(angles), jnp.cos(angles)], axis=1)

def place_embed(positions, columns):
    quarter = columns // 4
    omegas = 10000.0 ** (-jnp.arange(quarter, dtype=jnp.float32) / quarter)
    across = (positions // GRID_SIDE).astype(jnp.float32)[..., None] * omegas
    upward = (positions % GRID_SIDE).astype(jnp.float32)[..., None] * omegas
    return jnp.concatenate([jnp.sin(across), jnp.cos(across), jnp.sin(upward), jnp.cos(upward)], axis=-1)

def hyper_forward(wavelengths, relation, blending, widening, narrowing, shifting):
    highest = lax.Precision.HIGHEST
    columns = relation.shape[0]
    head_size = columns // HYP_HEADS
    embedded = wave_embed(wavelengths, columns)
    joined = jnp.dot(embedded, relation, precision=highest).reshape(embedded.shape[0], 3, HYP_HEADS, head_size)
    scores = jnp.einsum('bhd,chd->hbc', joined[:, 0], joined[:, 1], precision=highest) * head_size ** (-0.5)
    weights = jax.nn.softmax(scores, axis=-1)
    context = jnp.einsum('hbc,chd->bhd', weights, joined[:, 2], precision=highest).reshape(embedded.shape[0], columns)
    settled = normalize(embedded + jnp.dot(context, blending, precision=highest), 1e-05)
    widened = jax.nn.gelu(jnp.dot(settled, widening, precision=highest), approximate=False)
    hyper_out = normalize(settled + jnp.dot(widened, narrowing, precision=highest), 1e-05)
    bias_embed = jnp.dot(lax.optimization_barrier(jnp.mean(hyper_out, axis=0)), shifting, precision=highest)
    return (hyper_out, bias_embed)

def reference(patches, wavelengths, counts, positions, relation, blending, widening, narrowing, generator, shifting, scaling, centring, attending, offsets, merging, lifting, rescaling, recentring, expanding, priming, shrinking, settling, cotangent):
    highest = lax.Precision.HIGHEST
    weights = tuple((weight.astype(jnp.float32) for weight in (relation, blending, widening, narrowing, generator, shifting, scaling, centring, attending, offsets, merging, lifting, rescaling, recentring, expanding, priming, shrinking, settling)))
    pixels = patches.astype(jnp.float32)
    slot_index = jnp.arange(SLOTS)
    kept_rows = (slot_index[None, :] < counts[:, None]).astype(jnp.float32).reshape(TOKENS, 1)
    placed = place_embed(positions, D).reshape(TOKENS, D)
    head_size = D // HEADS

    def forward(pixels, params):
        w_rel, w_blend, w_wide, w_narrow, w_gen, w_shift, w_scale, w_centre, w_attend, w_offsets, w_merge, w_lift, w_rescale, w_recentre, w_expand, w_prime, w_shrink, w_settle = params
        hyper_out, bias_embed = hyper_forward(wavelengths, w_rel, w_blend, w_wide, w_narrow, w_shift)
        kernel = low(jnp.einsum('ch,phd->pcd', low(hyper_out), w_gen, precision=highest)).reshape(PIX * BANDS, D)
        start_rows = placed + bias_embed + low_back(jnp.dot(pixels, kernel, precision=highest))

        def block(inputs):
            residual, image_counts = inputs
            keys_valid = jnp.arange(SLOTS)[None, :] < image_counts[:, None]
            normed = low(normalize(residual, 1e-06) * w_scale + w_centre)
            joined = jnp.dot(normed, w_attend.reshape(D, 3 * D), precision=highest)
            split_shape = (IMG_DEV, SLOTS, HEADS, head_size)
            queries = both_round(joined[:, :D] + w_offsets[0]).reshape(split_shape)
            keys_all = both_round(joined[:, D:2 * D]).reshape(split_shape)
            values = both_round(joined[:, 2 * D:] + w_offsets[1]).reshape(split_shape)
            scores = low_back(jnp.einsum('ishd,ithd->ihst', queries, keys_all, precision=highest) * head_size ** (-0.5))
            scores = jnp.where(keys_valid[:, None, None, :], scores, -1000000000.0)
            attention = jax.nn.softmax(scores, axis=-1)
            context = both_round(jnp.einsum('ihst,ithd->ishd', low(attention), values, precision=highest)).reshape(IMG_DEV * SLOTS, D)
            middle = residual + low_back(jnp.dot(context, w_merge, precision=highest)) + w_lift
            second = low(normalize(middle, 1e-06) * w_rescale + w_recentre)
            widened = low_back(jnp.dot(second, w_expand, precision=highest) + w_prime)
            hidden = low(jax.nn.gelu(widened, approximate=False))
            return middle + low_back(jnp.dot(hidden, w_shrink, precision=highest)) + w_settle
        grouped = lax.map(jax.checkpoint(block), (start_rows.reshape(N_DP, IMG_DEV * SLOTS, D), counts.reshape(N_DP, IMG_DEV)))
        return grouped.reshape(TOKENS, D)
    result, pullback = jax.vjp(forward, pixels, weights)
    layer_out = (result * kept_rows).astype(jnp.bfloat16)
    patches_grad, weight_grads = pullback(cotangent.astype(jnp.float32) * kept_rows)
    relation_grad, blending_grad, widening_grad, narrowing_grad, generator_grad, shifting_grad, scaling_grad, centring_grad, attending_grad, offsets_grad, merging_grad, lifting_grad, rescaling_grad, recentring_grad, expanding_grad, priming_grad, shrinking_grad, settling_grad = weight_grads
    return (layer_out, patches_grad, relation_grad, blending_grad, widening_grad, narrowing_grad, generator_grad, shifting_grad, scaling_grad, centring_grad, attending_grad, offsets_grad, merging_grad, lifting_grad, rescaling_grad, recentring_grad, expanding_grad, priming_grad, shrinking_grad, settling_grad)
```

```python
from functools import partial

import jax
import jax.numpy as jnp
from jax import lax
from jax.experimental import pallas as pl
from jax.experimental.pallas import tpu as pltpu
from jax.sharding import PartitionSpec as P

HEADS = 12
HYP_HEADS = 4
GRID_SIDE = 14
MESH = pl.DeviceIdType.MESH
ANY = pl.BlockSpec(memory_space=pl.ANY)
VMEM = pl.BlockSpec(memory_space=pltpu.VMEM)


def normalize(values, epsilon):
    center = values - jnp.mean(values, axis=-1, keepdims=True)
    return center * lax.rsqrt(jnp.mean(center * center, axis=-1, keepdims=True) + epsilon)


def norm_parts(values, epsilon):
    center = values - jnp.mean(values, axis=-1, keepdims=True)
    inverse = lax.rsqrt(jnp.mean(center * center, axis=-1, keepdims=True) + epsilon)
    return (center * inverse, inverse)


def norm_backward(upstream, normed_rows, inverse, gain_row):
    scaled = upstream * gain_row
    return inverse * (
        scaled
        - jnp.mean(scaled, axis=-1, keepdims=True)
        - normed_rows * jnp.mean(scaled * normed_rows, axis=-1, keepdims=True)
    )


def wave_embed(wavelengths, columns):
    halfway = columns // 2
    omegas = 10000.0 ** (-jnp.arange(halfway, dtype=jnp.float32) / halfway)
    angles = wavelengths.astype(jnp.float32)[:, None] * 0.01 * omegas[None, :]
    return jnp.concatenate([jnp.sin(angles), jnp.cos(angles)], axis=1)


def place_embed(positions, columns):
    quarter = columns // 4
    omegas = 10000.0 ** (-jnp.arange(quarter, dtype=jnp.float32) / quarter)
    across = (positions // GRID_SIDE).astype(jnp.float32)[..., None] * omegas
    upward = (positions % GRID_SIDE).astype(jnp.float32)[..., None] * omegas
    return jnp.concatenate(
        [jnp.sin(across), jnp.cos(across), jnp.sin(upward), jnp.cos(upward)], axis=-1
    )


def hyper_forward(wavelengths, relation, blending, widening, narrowing, shifting):
    highest = lax.Precision.HIGHEST
    columns = relation.shape[0]
    head_size = columns // HYP_HEADS
    embedded = wave_embed(wavelengths, columns)
    joined = jnp.dot(embedded, relation, precision=highest).reshape(
        embedded.shape[0], 3, HYP_HEADS, head_size
    )
    scores = jnp.einsum(
        "bhd,chd->hbc", joined[:, 0], joined[:, 1], precision=highest
    ) * head_size ** (-0.5)
    weights = jax.nn.softmax(scores, axis=-1)
    context = jnp.einsum("hbc,chd->bhd", weights, joined[:, 2], precision=highest).reshape(
        embedded.shape[0], columns
    )
    settled = normalize(embedded + jnp.dot(context, blending, precision=highest), 1e-05)
    widened = jax.nn.gelu(jnp.dot(settled, widening, precision=highest), approximate=False)
    hyper_out = normalize(settled + jnp.dot(widened, narrowing, precision=highest), 1e-05)
    bias_embed = jnp.dot(jnp.mean(hyper_out, axis=0), shifting, precision=highest)
    return (hyper_out, bias_embed)


GROUP = 4


def by_head(block, lane_head):
    zero = jnp.zeros_like(block)
    return jnp.concatenate([jnp.where(lane_head == h, block, zero) for h in range(GROUP)], axis=0)


def own_blocks(product, lane_head, slots):
    total = jnp.where(lane_head == 0, product[:slots], 0.0)
    for h in range(1, GROUP):
        total = jnp.where(lane_head == h, product[h * slots : (h + 1) * slots], total)
    return total


NT = (((1,), (1,)), ((), ()))
TN = (((0,), (0,)), ((), ()))
NN = (((1,), (0,)), ((), ()))


def product(left, right, dims):
    return lax.dot_general(left, right, dims, preferred_element_type=jnp.float32)


def weights_of(keys, queries_wide, count, scale):
    scores = product(keys, queries_wide, NT) * scale
    slot = lax.broadcasted_iota(jnp.int32, scores.shape, 0)
    scores = jnp.where(slot < count, scores, -1000000000.0)
    raised = jnp.exp(scores - jnp.max(scores, axis=0, keepdims=True))
    return raised / jnp.sum(raised, axis=0, keepdims=True)


def attend_forward_kernel(width, head, counts_ref, joined_ref, context_ref):
    count = counts_ref[pl.program_id(0)]
    slots = joined_ref.shape[0]
    span = GROUP * head
    lane_head = lax.broadcasted_iota(jnp.int32, (slots, span), 1) // head
    for g in range(width // span):
        queries = joined_ref[:, g * span : (g + 1) * span]
        keys = joined_ref[:, width + g * span : width + (g + 1) * span]
        values = joined_ref[:, 2 * width + g * span : 2 * width + (g + 1) * span]
        weights = weights_of(keys, by_head(queries, lane_head), count, head**-0.5)
        wide = product(weights.astype(jnp.bfloat16), values, TN)
        context_ref[:, g * span : (g + 1) * span] = own_blocks(wide, lane_head, slots).astype(
            jnp.bfloat16
        )


def attend_backward_kernel(width, head, counts_ref, joined_ref, grad_ref, out_ref):
    count = counts_ref[pl.program_id(0)]
    slots = joined_ref.shape[0]
    span = GROUP * head
    scale = head**-0.5
    lane_head = lax.broadcasted_iota(jnp.int32, (slots, span), 1) // head
    for g in range(width // span):
        at_q = slice(g * span, (g + 1) * span)
        at_k = slice(width + g * span, width + (g + 1) * span)
        at_v = slice(2 * width + g * span, 2 * width + (g + 1) * span)
        keys = joined_ref[:, at_k]
        values = joined_ref[:, at_v]
        queries_wide = by_head(joined_ref[:, at_q], lane_head)
        grad_wide = by_head(grad_ref[:, at_q], lane_head)
        weights = weights_of(keys, queries_wide, count, scale)
        weights_grad = product(values, grad_wide, NT)
        out_ref[:, at_v] = product(weights.astype(jnp.bfloat16), grad_wide, NN).astype(
            jnp.bfloat16
        )
        inner = jnp.sum(weights * weights_grad, axis=0, keepdims=True)
        scores_grad = (weights * (weights_grad - inner)).astype(jnp.bfloat16)
        wide = product(scores_grad, keys, TN)
        out_ref[:, at_q] = (own_blocks(wide, lane_head, slots) * scale).astype(jnp.bfloat16)
        out_ref[:, at_k] = (product(scores_grad, queries_wide, NN) * scale).astype(jnp.bfloat16)


def attend_forward(counts, joined, slots):
    rows, width = joined.shape[0], joined.shape[1] // 3
    return pl.pallas_call(
        partial(attend_forward_kernel, width, width // HEADS),
        out_shape=jax.ShapeDtypeStruct((rows, width), jnp.bfloat16),
        grid_spec=pltpu.PrefetchScalarGridSpec(
            num_scalar_prefetch=1,
            grid=(rows // slots,),
            in_specs=[pl.BlockSpec((slots, 3 * width), lambda i, n: (i, 0))],
            out_specs=pl.BlockSpec((slots, width), lambda i, n: (i, 0)),
        ),
        name="attend_forward",
    )(counts, joined)


def attend_backward(counts, joined, context_grad, slots):
    rows, width = context_grad.shape
    return pl.pallas_call(
        partial(attend_backward_kernel, width, width // HEADS),
        out_shape=jax.ShapeDtypeStruct((rows, 3 * width), jnp.bfloat16),
        grid_spec=pltpu.PrefetchScalarGridSpec(
            num_scalar_prefetch=1,
            grid=(rows // slots,),
            in_specs=[
                pl.BlockSpec((slots, 3 * width), lambda i, n: (i, 0)),
                pl.BlockSpec((slots, width), lambda i, n: (i, 0)),
            ],
            out_specs=pl.BlockSpec((slots, 3 * width), lambda i, n: (i, 0)),
        ),
        name="attend_backward",
    )(counts, joined, context_grad)


class Place:
    def __init__(self):
        self.dp = lax.axis_index("dp")
        self.z = lax.axis_index("mp")
        self.core = self.dp % 2
        self.x = (self.dp // 2) % 2
        self.y = self.dp // 4
        self.dp_core = self.dp + 1 - 2 * self.core
        self.dp_x = self.dp + 2 - 4 * self.x
        self.dp_y = self.dp + 4 - 8 * self.y
        self.dp_both = self.dp_x + 4 - 8 * self.y

    def along_z(self, step):
        return (self.z + step) % 4

    def greet(self, z_steps=(1, 2, 3)):
        barrier = pltpu.get_barrier_semaphore()
        others = [(self.dp, self.along_z(step)) for step in z_steps]
        others += [(self.dp_core, self.z), (self.dp_x, self.z), (self.dp_y, self.z)]
        for other in others:
            pl.semaphore_signal(barrier, inc=1, device_id=other, device_id_type=MESH)
        pl.semaphore_wait(barrier, len(others))


class Sender:
    def __init__(self, sent, landed):
        self.sent, self.landed, self.started = sent, landed, []

    def __call__(self, source, target, device):
        k = len(self.started)
        copy = pltpu.make_async_remote_copy(
            src_ref=source,
            dst_ref=target,
            send_sem=self.sent.at[k],
            recv_sem=self.landed.at[k],
            device_id=device,
            device_id_type=MESH,
        )
        copy.start()
        self.started.append(copy)
        return copy

    def finish(self):
        for copy in self.started:
            copy.wait_send()


def spread_over_plane(put, me, at, own, first):
    half = own.shape[0] // 2
    low, high = pl.ds(0, half), pl.ds(half, half)
    mine = at(me.dp)
    by_x = put(own, mine, (me.dp_x, me.z))
    by_y = put(own, mine, (me.dp_y, me.z))
    by_core = [put(own, mine, (me.dp_core, me.z))]
    turned = []

    def pass_on():
        by_x.wait_recv()
        there = at(me.dp_x)
        turned.append(put(there.at[low], there.at[low], (me.dp_y, me.z)))
        by_core.append(put(there, there, (me.dp_core, me.z)))
        by_y.wait_recv()
        there = at(me.dp_y)
        turned.append(put(there.at[high], there.at[high], (me.dp_x, me.z)))
        by_core.append(put(there, there, (me.dp_core, me.z)))

    def last():
        for copy in turned:
            copy.wait_recv()
        there = at(me.dp_both)
        by_core.append(put(there, there, (me.dp_core, me.z)))
        return by_core

    return pass_on, last


def gather_kernel(
    part, w1, w2, w3, extra, whole, f1, f2, f3, extras, sent, landed, local
):
    me = Place()
    me.greet()
    put = Sender(sent, landed)
    keep = []

    def put_local(source, target):
        copy = pltpu.make_async_copy(source, target, local.at[len(keep)])
        copy.start()
        keep.append(copy)

    pieces = ((w1, f1), (w2, f2), (w3, f3))
    over_z = []
    steps = []
    mine = [put(part, whole.at[me.dp, me.z], (me.dp, me.along_z(r))) for r in (1, 2, 3)]
    steps.append(
        spread_over_plane(put, me, lambda dp: whole.at[dp, me.z], part, True)
    )
    over_z.append(mine)
    for weights, full in pieces:
        over_z.append(
            [
                put(weights.at[me.dp], full.at[me.z, me.dp], (me.dp, me.along_z(r)))
                for r in (1, 2, 3)
            ]
        )
    extra_over_z = [
        put(extra, extras.at[me.z], (me.dp, me.along_z(r))) for r in (1, 2, 3)
    ]
    put_local(part, whole.at[me.dp, me.z])
    put_local(extra, extras.at[me.z])
    for weights, full in pieces:
        put_local(weights, full.at[me.z])

    for index, copies in enumerate(over_z):
        for r, copy in zip((1, 2, 3), copies):
            copy.wait_recv()
            source = me.along_z(4 - r)
            if index == 0:
                at = lambda dp, source=source: whole.at[dp, source]
            else:
                full = pieces[index - 1][1]
                at = lambda dp, source=source, full=full: full.at[source, dp]
            steps.append(spread_over_plane(put, me, at, at(me.dp), False))
    for pass_on, _ in steps:
        pass_on()
    waiting = []
    for _, last in steps:
        waiting.extend(last())
    for copy in waiting + extra_over_z:
        copy.wait_recv()
    for copy in keep:
        copy.wait()
    put.finish()


def gather_all(part, pieces, extra):
    rows, columns = part.shape
    shape = jax.ShapeDtypeStruct
    low = jnp.bfloat16
    pieces = [p.reshape(8, p.shape[0] // 8, columns) for p in pieces]
    outs = [shape((8, 4, rows, columns), low)]
    outs += [shape((4,) + p.shape, low) for p in pieces]
    outs += [shape((4,) + extra.shape, low)]
    copies = 200
    return pl.pallas_call(
        gather_kernel,
        out_shape=outs,
        in_specs=[VMEM] * 5,
        out_specs=[ANY] * 5,
        scratch_shapes=[
            pltpu.SemaphoreType.DMA((copies,)),
            pltpu.SemaphoreType.DMA((copies,)),
            pltpu.SemaphoreType.DMA((5,)),
        ],
        compiler_params=pltpu.CompilerParams(collective_id=1, has_side_effects=True),
        name="gather_all",
    )(part, *pieces, extra)


def add_blocks(count, target, source, index_of, rows):
    def step(i, carry):
        at = index_of(i) + (rows, slice(None))
        total = target[at].astype(jnp.float32) + source[i].astype(jnp.float32)
        target[at] = total.astype(jnp.bfloat16)
        return carry

    lax.fori_loop(0, count, step, 0)


def reduce_kernel(
    gk, g1, g2, g3, ok, o1, o2, o3,
    acc, from_core, a1, b1, a2, b2, from_z, done, sent, landed, local, local_out,
):
    me = Place()
    me.greet()
    put = Sender(sent, landed)
    half = acc.shape[-2] // 2
    low, high = pl.ds(0, half), pl.ds(half, half)
    pieces = (gk, g1, g2, g3)
    outs = (ok, o1, o2, o3)
    state = [dict() for _ in pieces]

    def start(p):
        grads = pieces[p]
        copies, loads = [], []
        for z in range(4):
            if p == 0:
                give = grads.at[:, :, me.dp_core % 2, z]
                hold = grads.at[:, :, me.core, z]
            else:
                give = grads.at[z, :, :, me.dp_core % 2]
                hold = grads.at[z, :, :, me.core]
            copies.append(put(give, from_core.at[p, :, :, z], (me.dp_core, me.z)))
            load = pltpu.make_async_copy(hold, acc.at[p, :, :, z], local.at[4 * p + z])
            load.start()
            loads.append(load)
        state[p]["core"] = (copies, loads)

    def core(p):
        copies, loads = state[p]["core"]
        for z in range(4):
            loads[z].wait()
            copies[z].wait_recv()

        def step(i, carry):
            at = (p, i // 8, (i // 4) % 2, i % 4)
            total = acc[at].astype(jnp.float32) + from_core[at].astype(jnp.float32)
            acc[at] = total.astype(jnp.bfloat16)
            return carry

        lax.fori_loop(0, 16, step, 0)
        state[p]["a1"] = put(acc.at[p, :, 1 - me.x, :, low], a1.at[p], (me.dp_x, me.z))
        state[p]["b1"] = put(acc.at[p, 1 - me.y, :, :, high], b1.at[p], (me.dp_y, me.z))

    def plane_one(p):
        state[p]["a1"].wait_recv()

        def step_a(i, carry):
            at = (p, i // 4, me.x, i % 4, low)
            total = acc[at].astype(jnp.float32) + a1[p, i // 4, i % 4].astype(jnp.float32)
            acc[at] = total.astype(jnp.bfloat16)
            return carry

        lax.fori_loop(0, 8, step_a, 0)
        state[p]["a2"] = put(acc.at[p, 1 - me.y, me.x, :, low], a2.at[p], (me.dp_y, me.z))
        state[p]["b1"].wait_recv()

        def step_b(i, carry):
            at = (p, me.y, i // 4, i % 4, high)
            total = acc[at].astype(jnp.float32) + b1[p, i // 4, i % 4].astype(jnp.float32)
            acc[at] = total.astype(jnp.bfloat16)
            return carry

        lax.fori_loop(0, 8, step_b, 0)
        state[p]["b2"] = put(acc.at[p, me.y, 1 - me.x, :, high], b2.at[p], (me.dp_x, me.z))

    def plane_two(p):
        state[p]["a2"].wait_recv()
        state[p]["b2"].wait_recv()

        def step(z, carry):
            at = (p, me.y, me.x, z)
            first = acc[at + (low,)].astype(jnp.float32) + a2[p, z].astype(jnp.float32)
            acc[at + (low,)] = first.astype(jnp.bfloat16)
            second = acc[at + (high,)].astype(jnp.float32) + b2[p, z].astype(jnp.float32)
            acc[at + (high,)] = second.astype(jnp.bfloat16)
            return carry

        lax.fori_loop(0, 4, step, 0)
        state[p]["z"] = [
            put(
                acc.at[p, me.y, me.x, me.along_z(r)],
                from_z.at[p, r - 1],
                (me.dp, me.along_z(r)),
            )
            for r in (1, 2, 3)
        ]

    def along(p):
        for copy in state[p]["z"]:
            copy.wait_recv()
        total = acc[p, me.y, me.x, me.z].astype(jnp.float32)
        for r in range(3):
            total = total + from_z[p, r].astype(jnp.float32)
        if p == 0:
            ok[...] = total
        else:
            done[p - 1] = total.astype(jnp.bfloat16)
            out = outs[p]
            keep = pltpu.make_async_copy(done.at[p - 1], out.at[me.dp], local_out.at[p - 1])
            keep.start()
            state[p]["keep"] = keep
            state[p]["plane"] = spread_over_plane(
                put, me, lambda dp: out.at[dp], done.at[p - 1], False
            )

    def share(p):
        if p:
            state[p]["plane"][0]()

    def finish(p):
        if p:
            state[p]["last"] = state[p]["plane"][1]()

    stages = (core, plane_one, plane_two, along, share, finish)
    count = len(pieces)
    for p in range(count):
        start(p)
    for t in range(count + len(stages) - 1):
        for s in reversed(range(len(stages))):
            if 0 <= t - s < count:
                stages[s](t - s)
    for p in range(1, count):
        for copy in state[p]["last"]:
            copy.wait_recv()
        state[p]["keep"].wait()
    put.finish()


def reduce_all(kernel_grad, grads):
    columns = kernel_grad.shape[1]
    rows = kernel_grad.shape[0] // 32
    low, shape = jnp.bfloat16, jax.ShapeDtypeStruct
    half = rows // 2
    outs = [shape((rows, columns), jnp.float32)]
    outs += [shape((8, rows, columns), low)] * 3
    copies = 100
    return pl.pallas_call(
        reduce_kernel,
        out_shape=outs,
        in_specs=[ANY] * 4,
        out_specs=[VMEM] + [ANY] * 3,
        scratch_shapes=[
            pltpu.VMEM((4, 2, 2, 4, rows, columns), low),
            pltpu.VMEM((4, 2, 2, 4, rows, columns), low),
            pltpu.VMEM((4, 2, 4, half, columns), low),
            pltpu.VMEM((4, 2, 4, half, columns), low),
            pltpu.VMEM((4, 4, half, columns), low),
            pltpu.VMEM((4, 4, half, columns), low),
            pltpu.VMEM((4, 3, rows, columns), low),
            pltpu.VMEM((3, rows, columns), low),
            pltpu.SemaphoreType.DMA((copies,)),
            pltpu.SemaphoreType.DMA((copies,)),
            pltpu.SemaphoreType.DMA((16,)),
            pltpu.SemaphoreType.DMA((3,)),
        ],
        compiler_params=pltpu.CompilerParams(
            collective_id=2, has_side_effects=True, vmem_limit_bytes=60 * 1024 * 1024
        ),
        name="reduce_all",
    )(
        kernel_grad.reshape(2, 2, 2, 4, rows, columns),
        *(g.reshape(4, 2, 2, 2, rows, columns) for g in grads),
    )


def small_sum_kernel(values, total, buffers, incoming, sent, landed):
    me = Place()
    me.greet()
    put = Sender(sent, landed)
    partners = (
        (me.dp_core, me.z),
        (me.dp_x, me.z),
        (me.dp_y, me.z),
        (me.dp, me.z + 1 - 2 * (me.z % 2)),
        (me.dp, me.along_z(2)),
    )
    held = values
    for stage, partner in enumerate(partners):
        copy = put(held, incoming.at[stage], partner)
        copy.wait_recv()
        joined = held[...] + incoming[stage]
        if stage == len(partners) - 1:
            total[...] = joined
        else:
            buffers[stage] = joined
            held = buffers.at[stage]
    put.finish()


def small_sum(values):
    return pl.pallas_call(
        small_sum_kernel,
        out_shape=jax.ShapeDtypeStruct(values.shape, values.dtype),
        in_specs=[VMEM],
        out_specs=VMEM,
        scratch_shapes=[
            pltpu.VMEM((4,) + values.shape, values.dtype),
            pltpu.VMEM((5,) + values.shape, values.dtype),
            pltpu.SemaphoreType.DMA((5,)),
            pltpu.SemaphoreType.DMA((5,)),
        ],
        compiler_params=pltpu.CompilerParams(collective_id=3, has_side_effects=True),
        name="small_sum",
    )(values)


def body(
    sides,
    patches,
    wavelengths,
    counts,
    positions,
    relation,
    blending,
    widening,
    narrowing,
    generator,
    shifting,
    scaling,
    centring,
    attending,
    offsets,
    merging,
    lifting,
    rescaling,
    recentring,
    expanding,
    priming,
    shrinking,
    settling,
    cotangent,
):
    highest = lax.Precision.HIGHEST
    single = jnp.float32
    narrow = jnp.bfloat16
    direct = sides == (8, 4)
    shards = sides[1]
    local_rows = patches.shape[0]
    own_images = positions.shape[0]
    slot_count = positions.shape[1]
    model_width = merging.shape[1]
    local_width = merging.shape[0]
    local_hidden = priming.shape[0]
    my_index = lax.axis_index("mp")
    own_counts = lax.dynamic_slice_in_dim(counts, my_index * own_images, own_images)
    hyper_params = tuple(
        (weight.astype(single) for weight in (relation, blending, widening, narrowing, shifting))
    )
    (hyper_out, bias_embed), hyper_pullback = jax.vjp(
        partial(hyper_forward, wavelengths), *hyper_params
    )
    hyper_low = hyper_out.astype(narrow)
    kernel_part = jnp.einsum(
        "ch,phd->pcd", hyper_low, generator, preferred_element_type=single
    ).astype(narrow)
    part_shape = kernel_part.shape
    piece_rows = part_shape[0] * part_shape[1]
    piece_one = jnp.concatenate(
        [attending.transpose(1, 2, 0).reshape(3 * local_width, model_width), merging], axis=0
    )
    piece_two = expanding.T
    piece_three = shrinking
    extra = jnp.zeros((16, model_width), narrow)
    extra = extra.at[0, :local_hidden].set(priming)
    extra = extra.at[1:3, :local_width].set(offsets)
    kernel_flat = kernel_part.reshape(piece_rows, model_width)
    if direct:
        kernel_whole, one, two, three, extras = gather_all(
            kernel_flat, (piece_one, piece_two, piece_three), extra
        )
    else:
        kernel_whole = lax.all_gather(kernel_flat, ("dp", "mp"), axis=0, tiled=True)
        one, two, three, extras = (
            lax.all_gather(piece, "mp", axis=0)
            for piece in (piece_one, piece_two, piece_three, extra)
        )
    kernel_whole = kernel_whole.reshape(-1, model_width)
    one = one.reshape(shards, 4 * local_width, model_width)
    attend_rows = (
        one[:, : 3 * local_width]
        .reshape(shards, 3, local_width, model_width)
        .transpose(1, 0, 2, 3)
        .reshape(3 * model_width, model_width)
    )
    merge_rows = one[:, 3 * local_width :].reshape(model_width, model_width)
    expand_rows = two.reshape(-1, model_width)
    shrink_rows = three.reshape(-1, model_width)
    prime_all = extras[:, 0, :local_hidden].reshape(-1).astype(single)
    offsets_all = extras[:, 1:3, :local_width].transpose(1, 0, 2).reshape(2, model_width)
    attend_bias = jnp.concatenate(
        [offsets_all[0].astype(single), jnp.zeros((model_width,), single), offsets_all[1].astype(single)]
    )

    embedded = jnp.dot(patches, kernel_whole, preferred_element_type=single)
    kept_rows = (
        (jnp.arange(slot_count)[None, :] < own_counts[:, None])
        .astype(single)
        .reshape(local_rows, 1)
    )
    start_rows = (
        place_embed(positions, model_width).reshape(local_rows, model_width) + bias_embed + embedded
    )
    first_hat, first_inverse = norm_parts(start_rows, 1e-06)
    first_normed = (first_hat * scaling.astype(single) + centring.astype(single)).astype(narrow)
    joined = (product(first_normed, attend_rows, NT) + attend_bias).astype(narrow)
    context = attend_forward(own_counts, joined, slot_count)
    attended = product(context, merge_rows, NN)
    middle = start_rows + attended + lifting.astype(single)
    second_hat, second_inverse = norm_parts(middle, 1e-06)
    second_normed = (second_hat * rescaling.astype(single) + recentring.astype(single)).astype(
        narrow
    )
    widened = product(second_normed, expand_rows, NT) + prime_all
    below = 0.5 * (1.0 + lax.erf(widened * (0.5**0.5)))
    hidden = (widened * below).astype(narrow)
    slope = (
        below + widened * (jnp.exp(-0.5 * widened * widened) * (0.5 / jnp.pi) ** 0.5)
    ).astype(narrow)
    shrunk = product(hidden, shrink_rows, NN)
    result = middle + shrunk + settling.astype(single)
    layer_out = (result * kept_rows).astype(narrow)

    out_grad = cotangent.astype(single) * kept_rows
    out_low = out_grad.astype(narrow)
    settling_grad = jnp.sum(out_grad, axis=0)
    shrinking_grad = product(hidden, out_low, TN).astype(narrow)
    widened_grad = (product(out_low, shrink_rows, NT) * slope.astype(single)).astype(narrow)
    priming_grad = jnp.sum(widened_grad, axis=0, dtype=single)
    expanding_grad = product(widened_grad, second_normed, TN).astype(narrow)
    second_grad = product(widened_grad, expand_rows, NN)
    rescaling_grad = jnp.sum(second_grad * second_hat, axis=0)
    recentring_grad = jnp.sum(second_grad, axis=0)
    middle_grad = out_grad + norm_backward(
        second_grad, second_hat, second_inverse, rescaling.astype(single)
    )
    lifting_grad = jnp.sum(middle_grad, axis=0)
    middle_low = middle_grad.astype(narrow)
    merging_grad = product(context, middle_low, TN).astype(narrow)
    context_grad = product(middle_low, merge_rows, NT).astype(narrow)
    joined_grad = attend_backward(own_counts, joined, context_grad, slot_count)
    attending_grad = product(joined_grad, first_normed, TN).astype(narrow)
    bias_grad = jnp.sum(joined_grad, axis=0, dtype=single)
    first_grad = product(joined_grad, attend_rows, NN)
    scaling_grad = jnp.sum(first_grad * first_hat, axis=0)
    centring_grad = jnp.sum(first_grad, axis=0)
    start_grad = middle_grad + norm_backward(
        first_grad, first_hat, first_inverse, scaling.astype(single)
    )
    shift_total = jnp.sum(start_grad, axis=0)
    start_low = start_grad.astype(narrow)
    kernel_grad = product(patches, start_low, TN).astype(narrow)
    patches_grad = product(start_low, kernel_whole, NT)

    grad_one = jnp.concatenate(
        [
            attending_grad.reshape(3, shards, local_width, model_width)
            .transpose(1, 0, 2, 3)
            .reshape(shards, 3 * local_width, model_width),
            merging_grad.reshape(shards, local_width, model_width),
        ],
        axis=1,
    ).reshape(shards * 4 * local_width, model_width)
    if direct:
        kernel_sum, one, two, three = reduce_all(
            kernel_grad, (grad_one, expanding_grad, shrinking_grad)
        )
    else:
        kernel_sum = lax.psum_scatter(
            kernel_grad, ("dp", "mp"), scatter_dimension=0, tiled=True
        ).astype(single)
        one, two, three = (
            lax.psum(lax.psum_scatter(g, "mp", scatter_dimension=0, tiled=True), "dp")
            for g in (grad_one, expanding_grad, shrinking_grad)
        )
    one, two, three = (
        g.reshape(-1, model_width).astype(single) for g in (one, two, three)
    )
    attending_out = one[: 3 * local_width].reshape(3, local_width, model_width).transpose(2, 0, 1)
    merging_out = one[3 * local_width :]
    expanding_out = two.T
    shrinking_out = three

    kernel_sum = kernel_sum.reshape(part_shape)
    generator_grad = jnp.einsum(
        "ch,pcd->phd", hyper_low.astype(single), kernel_sum, precision=highest
    )
    hyper_part = jnp.einsum("pcd,phd->ch", kernel_sum, generator.astype(single), precision=highest)
    vectors = (
        hyper_part,
        scaling_grad,
        centring_grad,
        rescaling_grad,
        recentring_grad,
        lifting_grad,
        settling_grad,
        shift_total,
        bias_grad[:model_width],
        bias_grad[2 * model_width :],
        priming_grad,
    )
    if direct:
        flat = jnp.concatenate([v.reshape(-1, 128) for v in vectors], axis=0)
        lines = flat.shape[0]
        flat = jnp.pad(flat, ((0, -lines % 8), (0, 0)))
        summed = small_sum(flat)
        totals, at = [], 0
        for v in vectors:
            n = v.size // 128
            totals.append(summed[at : at + n].reshape(v.shape))
            at += n
    else:
        totals = lax.psum(vectors, ("dp", "mp"))
    (
        hyper_part,
        scaling_grad,
        centring_grad,
        rescaling_grad,
        recentring_grad,
        lifting_grad,
        settling_grad,
        shift_total,
        query_bias,
        value_bias,
        priming_grad,
    ) = totals
    offsets_grad = lax.dynamic_slice_in_dim(
        jnp.stack([query_bias, value_bias]), my_index * local_width, local_width, axis=1
    )
    priming_grad = lax.dynamic_slice_in_dim(priming_grad, my_index * local_hidden, local_hidden)
    relation_grad, blending_grad, widening_grad, narrowing_grad, shifting_grad = hyper_pullback(
        (hyper_part, shift_total)
    )
    return (
        layer_out,
        patches_grad,
        relation_grad,
        blending_grad,
        widening_grad,
        narrowing_grad,
        generator_grad,
        shifting_grad,
        scaling_grad,
        centring_grad,
        attending_out,
        offsets_grad,
        merging_out,
        lifting_grad,
        rescaling_grad,
        recentring_grad,
        expanding_out,
        priming_grad,
        shrinking_out,
        settling_grad,
    )


def solution(mesh):
    placed = (
        P(("dp", "mp"), None),
        P(),
        P("dp"),
        P(("dp", "mp"), None),
        P(),
        P(),
        P(),
        P(),
        P(("dp", "mp"), None, None),
        P(),
        P(),
        P(),
        P(None, None, "mp"),
        P(None, "mp"),
        P("mp", None),
        P(),
        P(),
        P(),
        P(None, "mp"),
        P("mp"),
        P("mp", None),
        P(),
        P(("dp", "mp"), None),
    )
    return jax.shard_map(
        partial(body, (mesh.shape["dp"], mesh.shape["mp"])),
        mesh=mesh,
        in_specs=placed,
        out_specs=(
            P(("dp", "mp"), None),
            P(("dp", "mp"), None),
            P(),
            P(),
            P(),
            P(),
            P(("dp", "mp"), None, None),
            P(),
            P(),
            P(),
            P(None, None, "mp"),
            P(None, "mp"),
            P("mp", None),
            P(),
            P(),
            P(),
            P(None, "mp"),
            P("mp"),
            P("mp", None),
            P(),
        ),
        check_vma=False,
    )
```
